32 devices in a mesh: gy: 8 (over z, x), gx: 4 (over y, core).
Axes of the slice: x: 2, y: 2, z: 4, core: 2. Of those that a mesh axis runs over, the one named last changes fastest.
Arguments:
- imbalance: float32 [4, 1024, 2048], P(None, 'gy', 'gx'), may hold values from -9 to 9
- flow: float32 [2, 4, 1024, 2048], P(None, None, 'gy', 'gx'), may hold values from -3 to 3
- potential: float32 [4, 1024, 2048], P(None, 'gy', 'gx'), may hold values from -5 to 5
- cost: float32 [1024, 2048], P('gy', 'gx'), may hold values from 0.2 to 2
Outputs:
- flow_out: float32 [2, 4, 1024, 2048], P(None, None, 'gy', 'gx')
- potential_out: float32 [4, 1024, 2048], P(None, 'gy', 'gx')
- residual: float32 [4], replicated
The draws below stay inside these ranges and needn't reach their ends.
All inputs are finite; a program needn't handle non-finite values.
Results may differ from the reference program's by a relative error of at most 0.0001.
Values sent between devices are 32-bit elements; how exact they have to be, the bound alone decides.
A program may use at most 64 MiB of HBM per device.

```python
import math
from functools import partial
import jax
import jax.numpy as jnp
from jax import lax

PAIRS = 4
ITERS = 12
NR = 1024
NC = 2048


def draw_imbalance(key, part):
    row_pos = jnp.arange(NR, dtype=jnp.float32) / max(NR - 1, 1)
    col_pos = jnp.arange(NC, dtype=jnp.float32) / max(NC - 1, 1)
    envelope = 0.25 * (1.0 + 2.0 * row_pos)[:, None] * (1.0 + 2.0 * col_pos)[None, :]
    values = envelope * jnp.clip(jax.random.normal(key, (PAIRS, NR, NC), jnp.float32), -3.5, 3.5)
    return jnp.clip(values, -9.0, 9.0)


def shard_levels(rng, extent, cuts, low, largest):
    loudness = 1.0
    for dim, shards_of in cuts:
        draws = jax.random.uniform(jax.random.fold_in(jax.random.fold_in(rng, 6), dim), (shards_of,), jnp.float32, low / len(cuts), largest / len(cuts))
        loudness = loudness * jnp.repeat(jnp.exp(draws), extent[dim] // shards_of).reshape((-1,) + (1,) * (len(extent) - 1 - dim))
    return loudness


def centred(own_key, dims, spread, bound, pieces=(), held_as=jnp.bfloat16):
    array = jax.random.normal(own_key, dims, jnp.float32) * spread
    if len(pieces) > 0:
        array = shard_levels(own_key, dims, pieces, -0.22, 0.18) * array
    return jnp.clip(array, min=-bound, max=bound).astype(held_as)


def setup_inputs(seed: int = 0) -> dict:
    arg_keys = jax.random.split(jax.random.key(seed), 5)
    imbalance = draw_imbalance(jax.random.fold_in(arg_keys[4], 71), 0)
    flow = centred(arg_keys[1], (2, PAIRS, NR, NC), 0.5, 3.0, ((2, 8), (3, 4)), jnp.float32)
    potential = centred(arg_keys[2], (PAIRS, NR, NC), 1.0, 5.0, ((1, 8), (2, 4)), jnp.float32)
    cost = jnp.clip(jnp.exp(math.log(2.0) - 2.3025851 * jax.random.uniform(arg_keys[3], (NR, NC), jnp.float32) ** shard_levels(arg_keys[3], (NR, NC), ((0, 8), (1, 4)), -0.2, 0.2)), 0.2, 2.0)
    return {"imbalance": imbalance, "flow": flow, "potential": potential, "cost": cost}


initial_step = 0.35
epsilon = 1e-06

def gradient(potential):
    from_below = jnp.concatenate([potential[1:], jnp.zeros_like(potential[:1])], 0)
    from_right = jnp.concatenate([potential[:, 1:], jnp.zeros_like(potential[:, :1])], 1)
    return (from_below - potential, from_right - potential)

def divergence(flow_down, flow_right):
    from_above = jnp.concatenate([jnp.zeros_like(flow_down[:1]), flow_down[:-1]], 0)
    from_left = jnp.concatenate([jnp.zeros_like(flow_right[:, :1]), flow_right[:, :-1]], 1)
    return flow_down - from_above + flow_right - from_left

def shrink(moved_down, moved_right, threshold):
    magnitude = jnp.sqrt(moved_down * moved_down + moved_right * moved_right)
    factor = jnp.maximum(magnitude - threshold, 0.0) / jnp.maximum(magnitude, threshold)
    return (factor * moved_down, factor * moved_right)

def solve_pair(arrays, cost):
    source, flow_down, flow_right, potential = arrays
    primal_rate = jnp.full((), initial_step, jnp.float32)
    dual_rate = jnp.full((), initial_step, jnp.float32)
    spread_old = divergence(flow_down, flow_right)
    for iteration in range(ITERS):
        slope_down, slope_right = gradient(potential)
        new_down, new_right = shrink(flow_down + primal_rate * slope_down, flow_right + primal_rate * slope_right, primal_rate * cost)
        spread_new = divergence(new_down, new_right)
        new_potential = potential + dual_rate * (2.0 * spread_new - spread_old - source)
        if iteration + 1 < ITERS:
            diff_down = new_down - flow_down
            diff_right = new_right - flow_right
            primal_change = jnp.sum(diff_down * diff_down + diff_right * diff_right)
            change = new_potential - potential
            dual_change = jnp.sum(change * change)
            rescale = jnp.sqrt(jnp.sqrt((primal_change + epsilon) / (dual_change + epsilon)))
            primal_rate = primal_rate / rescale
            dual_rate = dual_rate * rescale
        flow_down, flow_right, potential, spread_old = (new_down, new_right, new_potential, spread_new)
    shortfall = spread_old - source
    residual = jnp.sum(shortfall * shortfall) / (NR * NC)
    return (flow_down, flow_right, potential, residual)

def reference(imbalance, flow, potential, cost):
    result_down, result_right, result_potential, residual = lax.map(partial(solve_pair, cost=cost), (imbalance, flow[0], flow[1], potential))
    return (jnp.stack([result_down, result_right]), result_potential, residual)
```

```python
import functools

import jax
import jax.numpy as jnp
from jax import lax
from jax.experimental import pallas as pl
from jax.experimental.pallas import tpu as pltpu
from jax.sharding import PartitionSpec as P

ITERS = 12
LANES = 128
SUBS = 8

initial_step = 0.35
epsilon = 1e-06
MESH = pl.DeviceIdType.MESH


def kernel(
    ny, nx,
    imb_hbm, flow_hbm, u_hbm, cost_hbm,
    flow_hbm_out, u_hbm_out, res_out,
    imb_in, flow_in, u_in, cost_in,
    A, B, U, R, IM, CO,
    tau_ref, sig_ref,
    row_send, col_send, row_recv, col_recv, msg_send, msg_recv,
    ext_row, ext_col, ext_row_in, ext_col_in, grow, gcol,
    halo_ssem, halo_rsem, msg_ssem, msg_rsem, ext_ssem, ext_rsem, in_sem, out_sem,
):
    pairs, T, _, C = A.shape
    n = ny * nx
    gy, gx = lax.axis_index("gy"), lax.axis_index("gx")
    me = gy * nx + gx
    up, down, left, right = gy > 0, gy < ny - 1, gx > 0, gx < nx - 1
    f32 = jnp.float32

    K = C // LANES

    def column(ref, k):
        return ref.at[(slice(None),) * (len(ref.shape) - 1) + (pl.ds(k * LANES, LANES),)]

    fetches = [
        pltpu.make_async_copy(column(src, k), dst.at[k], in_sem.at[i, k])
        for i, (src, dst) in enumerate(((cost_hbm, cost_in), (u_hbm, u_in), (flow_hbm, flow_in), (imb_hbm, imb_in)))
        for k in range(K)
    ]
    for copy in fetches:
        copy.start()

    def gather(ref, *index):
        rows = pl.ds(index[-1], SUBS, stride=T)
        return jnp.concatenate([ref[(k,) + index[:-1] + (rows, slice(None))] for k in range(K)], axis=1)

    def scatter(ref, value, *index):
        rows = pl.ds(index[-1], SUBS, stride=T)
        for k in range(K):
            ref[(k,) + index[:-1] + (rows, slice(None))] = value[:, k * LANES:(k + 1) * LANES]

    barrier = pltpu.get_barrier_semaphore()

    def coords(offset):
        other = lax.rem(me + offset, n)
        return (other // nx, lax.rem(other, nx))

    def greet(k, c):
        pl.semaphore_signal(barrier, inc=1, device_id=coords(k), device_id_type=MESH)
        return c

    lax.fori_loop(1, n, greet, 0)

    lane = lax.broadcasted_iota(jnp.int32, (SUBS, LANES), 1)
    sub = lax.broadcasted_iota(jnp.int32, (SUBS, LANES), 0)
    subw = lax.broadcasted_iota(jnp.int32, (SUBS, C), 0)
    group, within = lane // T, lax.rem(lane, T)
    lane1, within1 = lane[0:1], within[0:1]

    def wide(x):
        return jnp.concatenate([x] * (C // LANES), axis=1)

    def row8(x, width):
        return jnp.broadcast_to(x, (SUBS, width))

    def to_left(x, entering):
        r = pltpu.roll(x, C - 1, 1)
        lanes = lax.broadcasted_iota(jnp.int32, entering.shape, 1)
        tail = jnp.where(lanes == LANES - 1, entering, r[:, C - LANES:])
        return jnp.concatenate([r[:, : C - LANES], tail], axis=1)

    def to_right(x, entering):
        r = pltpu.roll(x, 1, 1)
        head = jnp.where(lane == 0, entering, r[:, :LANES])
        return jnp.concatenate([head, r[:, LANES:]], axis=1)

    def pack_first(acc, x, t):
        v = x[:, :LANES]
        return jnp.where(lane == t, pltpu.roll(v, t, 1) if t else v, acc)

    def pack_last(acc, x, t):
        v = pltpu.roll(x[:, C - LANES:], (t + 1) % LANES, 1)
        return jnp.where(lane == t, v, acc)

    def place(acc, packed, p):
        return jnp.where(group == p, pltpu.roll(packed, p * T, 1), acc)

    def remote(src, dst, ssem, rsem, where):
        return pltpu.make_async_remote_copy(
            src_ref=src, dst_ref=dst, send_sem=ssem, recv_sem=rsem, device_id=where, device_id_type=MESH
        )

    def halos(slot):
        rows = [
            (ok_to, ok_from, remote(row_send.at[slot, k], row_recv.at[slot, k], halo_ssem.at[slot, k], halo_rsem.at[slot, k], (gy + d, gx)))
            for k, d, ok_to, ok_from in ((0, -1, up, down), (1, 1, down, up))
        ]
        cols = [
            (ok_to, ok_from, remote(col_send.at[slot, k], col_recv.at[slot, k], halo_ssem.at[slot, 2 + k], halo_rsem.at[slot, 2 + k], (gy, gx + d)))
            for k, d, ok_to, ok_from in ((0, -1, left, right), (1, 1, right, left))
        ]
        return rows + cols

    def extras():
        return [
            (down, up, remote(ext_row, ext_row_in, ext_ssem.at[0], ext_rsem.at[0], (gy + 1, gx))),
            (right, left, remote(ext_col, ext_col_in, ext_ssem.at[1], ext_rsem.at[1], (gy, gx + 1))),
        ]

    def start_all(copies):
        for ok_to, _, copy in copies:
            @pl.when(ok_to)
            def _(copy=copy):
                copy.start()

    def wait_all(copies):
        for ok_to, ok_from, copy in copies:
            @pl.when(ok_from)
            def _(copy=copy):
                copy.wait_recv()

            @pl.when(ok_to)
            def _(copy=copy):
                copy.wait_send()

    def send_message(slot, row):
        msg_send[slot] = row
        msg_recv[slot, me] = row

        def send(k, c):
            remote(msg_send.at[slot], msg_recv.at[slot, me], msg_ssem.at[slot], msg_rsem.at[slot], coords(k)).start()
            return c

        lax.fori_loop(1, n, send, 0)

    def wait_message(slot):
        whole = msg_recv.at[slot, pl.ds(0, n - 1)]
        pltpu.make_async_copy(whole, whole, msg_rsem.at[slot]).wait()
        pltpu.make_async_copy(whole, whole, msg_ssem.at[slot]).wait()

    def total_rows(slot):
        parts = [msg_recv[slot, k] for k in range(n)]
        while len(parts) > 1:
            parts = [sum(parts[k + 1:k + 2], parts[k]) for k in range(0, len(parts), 2)]
        total = row8(parts[0], LANES)
        pick = jnp.where(sub < pairs, sub * T + 1, (sub - pairs) * T + 2)
        return row8_lanes(jnp.sum(jnp.where(lane == pick, total, 0.0), axis=1, keepdims=True))

    def row8_lanes(x):
        return jnp.broadcast_to(x, (SUBS, LANES))

    def message(first, last, sums_a, sums_b):
        return jnp.where(
            within1 == T - 1, first[SUBS - 1:SUBS],
            jnp.where(within1 == 0, last[0:1], jnp.where(within1 == 1, sums_a, sums_b)),
        )

    ones = jnp.ones((SUBS, LANES), f32)
    for copy in fetches:
        copy.wait()
    for t in range(T):
        CO[t] = gather(cost_in, t)

    def load(p, carry):
        packs = [ones] * 5
        for t in range(T):
            a, b = gather(flow_in, 0, p, t), gather(flow_in, 1, p, t)
            u = gather(u_in, p, t)
            A[p, t] = a
            B[p, t] = b
            U[p, t] = u
            IM[p, t] = gather(imb_in, p, t)
            packs[0] = pack_first(packs[0], u, t)
            for k, x in ((1, u), (2, a), (3, b), (4, CO[t])):
                packs[k] = pack_last(packs[k], x, t)
            if t == 0:
                row_send[0, 0, pl.ds(p, 1), :] = u[0:1]
            if t == T - 1:
                row_send[0, 1, pl.ds(p, 1), :] = u[SUBS - 1:]
                ext_row[0, pl.ds(p, 1), :] = a[SUBS - 1:]
                ext_row[1, pl.ds(p, 1), :] = b[SUBS - 1:]
                ext_row[2, pl.ds(p, 1), :] = CO[t][SUBS - 1:]
        return tuple(place(c, x, p) for c, x in zip(carry, packs))

    first, last, last_a, last_b, last_c = lax.fori_loop(0, pairs, load, (ones,) * 5)
    col_send[0, 0] = first
    col_send[0, 1] = last
    ext_col[0] = last_a
    ext_col[1] = last_b
    ext_col[2] = last_c
    tau_ref[...] = jnp.full((SUBS, LANES), initial_step, f32)
    sig_ref[...] = jnp.full((SUBS, LANES), initial_step, f32)

    for missing, refs in (
        (jnp.logical_not(down), [row_recv.at[s, 0] for s in range(2)]),
        (jnp.logical_not(up), [row_recv.at[s, 1] for s in range(2)] + [ext_row_in]),
        (jnp.logical_not(right), [col_recv.at[s, 0] for s in range(2)]),
        (jnp.logical_not(left), [col_recv.at[s, 1] for s in range(2)] + [ext_col_in]),
    ):
        @pl.when(missing)
        def _(refs=refs):
            for ref in refs:
                ref[...] = jnp.zeros(ref.shape, f32)

    pl.semaphore_wait(barrier, n - 1)
    start_all(extras())
    start_all(halos(0))
    send_message(0, message(first, last, ones[0:1], ones[0:1]))
    wait_all(extras())
    grow[...] = ext_row_in[0:2]
    gcol[...] = ext_col_in[0:2]

    def above_first(a_last, p):
        ghost = row8(grow[0, pl.ds(p, 1), :], C)
        return jnp.where(subw == 0, ghost, pltpu.roll(a_last, 1, 0))

    def shortfall(p, t, a, a_above, b, gb):
        b_left = to_right(b, pltpu.roll(gb, (LANES - t) % LANES, 1))
        return ((a - a_above) + (b - b_left)) - IM[p, t]

    def ghost_flux(p):
        return pltpu.roll(gcol[1], lax.rem(LANES - p * T, LANES), 1)

    def begin(p, c):
        gb = ghost_flux(p)
        for t in range(T):
            above = A[p, t - 1] if t else above_first(A[p, T - 1], p)
            R[p, t] = shortfall(p, t, A[p, t], above, B[p, t], gb)
        return c

    lax.fori_loop(0, pairs, begin, 0)
    wait_all(halos(0))
    wait_message(0)

    results = [
        pltpu.make_async_copy(src.at[k], column(dst, k), out_sem.at[i, k])
        for i, (src, dst) in enumerate(((flow_in, flow_hbm_out), (u_in, u_hbm_out)))
        for k in range(K)
    ]

    def shrink(va, vb, t):
        f = jnp.maximum(1.0 - t * lax.rsqrt(va * va + vb * vb), 0.0)
        return f * va, f * vb

    def ghosts(slot):
        u = row_recv[slot, 1]
        sub_p, lane_p = sub[:pairs], lane[:pairs]
        ok = jnp.logical_and(up, right)
        corner = msg_recv[slot, jnp.where(ok, me - nx + 1, me)]
        corner = jnp.where(ok, corner, jnp.zeros_like(corner))
        corner = jnp.broadcast_to(corner, (pairs, LANES))
        corner = jnp.sum(jnp.where(lane_p == sub_p * T + T - 1, corner, 0.0), axis=1, keepdims=True)
        u_right = to_left(u, jnp.broadcast_to(corner, (pairs, LANES)))
        rate = wide(tau_ref[0:pairs])
        a2, b2 = shrink(
            grow[0] + rate * (row_send[slot, 0] - u), grow[1] + rate * (u_right - u), rate * ext_row_in[2]
        )
        grow[0] = jnp.where(up, a2, jnp.zeros_like(a2))
        grow[1] = jnp.where(up, b2, jnp.zeros_like(b2))
        u = col_recv[slot, 1]
        ok = jnp.logical_and(down, left)
        corner = msg_recv[slot, jnp.where(ok, me + nx - 1, me)]
        corner = jnp.where(ok, corner, jnp.zeros_like(corner))
        turn = jnp.where(sub == SUBS - 1, row8(corner, LANES), pltpu.roll(u, SUBS - 1, 0))
        u_down = jnp.where(within == T - 1, pltpu.roll(turn, T - 1, 1), pltpu.roll(u, LANES - 1, 1))
        rate = row8(tau_ref[0:1], LANES)
        for p in range(1, pairs):
            rate = jnp.where(group == p, row8(tau_ref[p:p + 1], LANES), rate)
        a2, b2 = shrink(
            gcol[0] + rate * (u_down - u), gcol[1] + rate * (col_send[slot, 0] - u), rate * ext_col_in[2]
        )
        gcol[0] = jnp.where(left, a2, jnp.zeros_like(a2))
        gcol[1] = jnp.where(left, b2, jnp.zeros_like(b2))

    def sweep(slot, closing):
        other = 1 - slot
        ghosts(slot)

        def problem(p, carry):
            sums_a, sums_b, first, last = carry
            tau = wide(row8(tau_ref[pl.ds(p, 1), :], LANES))
            sigma = wide(row8(sig_ref[pl.ds(p, 1), :], LANES))
            gb = ghost_flux(p)
            hc = pltpu.roll(col_recv[slot, 0], LANES - 1 - p * T, 1)
            acc_p = jnp.zeros((SUBS, C), f32)
            acc_d = jnp.zeros((SUBS, C), f32)
            pack_f, pack_l = ones, ones

            def dual(t, a2, above, b2, u):
                nonlocal acc_p, acc_d, pack_f, pack_l
                r2 = shortfall(p, t, a2, above, b2, gb)
                change = sigma * (r2 + (r2 - R[p, t]))
                u2 = u + change
                if closing:
                    acc_d = acc_d + r2 * r2
                    scatter(u_in, u2, p, t)
                    return
                acc_d = acc_d + change * change
                R[p, t] = r2
                U[p, t] = u2
                pack_f = pack_first(pack_f, u2, t)
                pack_l = pack_last(pack_l, u2, t)
                if t == 0:
                    row_send[other, 0, pl.ds(p, 1), :] = u2[0:1]
                if t == T - 1:
                    row_send[other, 1, pl.ds(p, 1), :] = u2[SUBS - 1:]

            u_first = u = U[p, 0]
            for t in range(T):
                if t < T - 1:
                    u_down = U[p, t + 1]
                else:
                    below = row8(row_recv[slot, 0, pl.ds(p, 1), :], C)
                    u_down = jnp.where(subw == SUBS - 1, below, pltpu.roll(u_first, SUBS - 1, 0))
                u_right = to_left(u, pltpu.roll(hc, (LANES - t) % LANES, 1))
                a, b = A[p, t], B[p, t]
                a2, b2 = shrink(a + tau * (u_down - u), b + tau * (u_right - u), tau * CO[t])
                if closing:
                    scatter(flow_in, a2, 0, p, t)
                    scatter(flow_in, b2, 1, p, t)
                else:
                    A[p, t] = a2
                    B[p, t] = b2
                    da, db = a2 - a, b2 - b
                    acc_p = acc_p + (da * da + db * db)
                if t:
                    dual(t, a2, above, b2, u)
                else:
                    a_first, b_first = a2, b2
                above, u = a2, u_down
            dual(0, a_first, above_first(above, p), b_first, u_first)

            def settle(sums, acc):
                part = jnp.sum(jnp.sum(acc, axis=0, keepdims=True), axis=1, keepdims=True)
                return jnp.where(group[0:1] == p, jnp.broadcast_to(part, (1, LANES)), sums)

            sums_b = settle(sums_b, acc_d)
            if closing:
                return sums_a, sums_b, first, last
            return settle(sums_a, acc_p), sums_b, place(first, pack_f, p), place(last, pack_l, p)

        start = (ones[0:1], ones[0:1], ones, ones)
        sums_a, sums_b, first, last = lax.fori_loop(0, pairs, problem, start)
        if not closing:
            col_send[other, 0] = first
            col_send[other, 1] = last
            start_all(halos(other))
        send_message(other, message(first, last, sums_a, sums_b))
        if closing:
            for copy in results:
                copy.start()
        else:
            wait_all(halos(other))
        wait_message(other)
        return total_rows(other)

    def turn(i, c):
        sums = sweep(lax.rem(i, 2), False)
        primal, dual = sums, pltpu.roll(sums, SUBS - pairs, 0)
        s = jnp.sqrt(jnp.sqrt((primal + epsilon) / (dual + epsilon)))
        tau_ref[...] = tau_ref[...] / s
        sig_ref[...] = sig_ref[...] * s
        return c

    lax.fori_loop(0, ITERS - 1, turn, 0)
    sums = sweep((ITERS - 1) % 2, True)
    cells = T * SUBS * C * n
    res_out[...] = sums / cells
    for copy in results:
        copy.wait()


def local(ny, nx, imbalance, flow, potential, cost):
    pairs, rows, cols = imbalance.shape
    T = rows // SUBS
    n = ny * nx
    assert 2 * pairs == SUBS and pairs * T <= LANES and T >= 4
    f32 = jnp.float32
    block = (pairs, T, SUBS, cols)
    packed = (SUBS, LANES)
    K = cols // LANES
    hbm = pl.BlockSpec(memory_space=pltpu.HBM)
    flow_out, u_out, res = pl.pallas_call(
        functools.partial(kernel, ny, nx),
        out_shape=(
            jax.ShapeDtypeStruct(flow.shape, f32),
            jax.ShapeDtypeStruct(potential.shape, f32),
            jax.ShapeDtypeStruct(packed, f32),
        ),
        in_specs=[hbm] * 4,
        out_specs=(hbm, hbm, pl.BlockSpec(memory_space=pltpu.VMEM)),
        scratch_shapes=[
            pltpu.VMEM((K, pairs, rows, LANES), f32), pltpu.VMEM((K, 2, pairs, rows, LANES), f32),
            pltpu.VMEM((K, pairs, rows, LANES), f32), pltpu.VMEM((K, rows, LANES), f32),
            pltpu.VMEM(block, f32), pltpu.VMEM(block, f32), pltpu.VMEM(block, f32), pltpu.VMEM(block, f32),
            pltpu.VMEM(block, f32), pltpu.VMEM(block[1:], f32),
            pltpu.VMEM(packed, f32), pltpu.VMEM(packed, f32),
            pltpu.VMEM((2, 2, pairs, cols), f32), pltpu.VMEM((2, 2) + packed, f32),
            pltpu.VMEM((2, 2, pairs, cols), f32), pltpu.VMEM((2, 2) + packed, f32),
            pltpu.VMEM((2, 1, LANES), f32), pltpu.VMEM((2, n, 1, LANES), f32),
            pltpu.VMEM((3, pairs, cols), f32), pltpu.VMEM((3,) + packed, f32),
            pltpu.VMEM((3, pairs, cols), f32), pltpu.VMEM((3,) + packed, f32),
            pltpu.VMEM((2, pairs, cols), f32), pltpu.VMEM((2,) + packed, f32),
            pltpu.SemaphoreType.DMA((2, 4)), pltpu.SemaphoreType.DMA((2, 4)),
            pltpu.SemaphoreType.DMA((2,)), pltpu.SemaphoreType.DMA((2,)),
            pltpu.SemaphoreType.DMA((2,)), pltpu.SemaphoreType.DMA((2,)),
            pltpu.SemaphoreType.DMA((4, K)), pltpu.SemaphoreType.DMA((2, K)),
        ],
        compiler_params=pltpu.CompilerParams(
            collective_id=0, has_side_effects=True, vmem_limit_bytes=48 * 1024 * 1024
        ),
    )(imbalance, flow, potential, cost)
    return flow_out, u_out, res[pairs:, 0]


def solution(mesh):
    placed = (P(None, "gy", "gx"), P(None, None, "gy", "gx"), P(None, "gy", "gx"), P("gy", "gx"))
    return jax.shard_map(
        functools.partial(local, mesh.shape["gy"], mesh.shape["gx"]),
        mesh=mesh,
        in_specs=placed,
        out_specs=(P(None, None, "gy", "gx"), P(None, "gy", "gx"), P()),
        check_vma=False,
    )
```

```python
import functools

import jax
import jax.numpy as jnp
from jax import lax
from jax.experimental import pallas as pl
from jax.experimental.pallas import tpu as pltpu
from jax.sharding import PartitionSpec as P

ITERS = 12
LANES = 128
GROUPS = 4
SUBS = 8

initial_step = 0.35
epsilon = 1e-06
MESH = pl.DeviceIdType.MESH


def kernel(
    ny, nx,
    imb_hbm, flow_hbm, u_hbm, cost_hbm,
    flow_hbm_out, u_hbm_out, res_out,
    imb_in, flow_in, u_in, cost_in,
    A, B, U, R, IM, CO,
    tau_ref, sig_ref,
    row_send, col_send, row_recv, col_recv, msg_send, msg_recv,
    ext_row, ext_col, ext_row_in, ext_col_in, grow, gcol,
    halo_ssem, halo_rsem, msg_ssem, msg_rsem, ext_ssem, ext_rsem, in_sem, out_sem,
):
    pairs, T, _, C = A.shape
    n = ny * nx
    G = grow.shape[0]
    gp = pairs // G
    gy, gx = lax.axis_index("gy"), lax.axis_index("gx")
    me = gy * nx + gx
    up, down, left, right = gy > 0, gy < ny - 1, gx > 0, gx < nx - 1
    f32 = jnp.float32

    K = C // LANES

    def column(ref, k):
        return ref.at[(slice(None),) * (len(ref.shape) - 1) + (pl.ds(k * LANES, LANES),)]

    fetches = [
        pltpu.make_async_copy(column(src, k), dst.at[k], in_sem.at[i, k])
        for i, (src, dst) in enumerate(((cost_hbm, cost_in), (u_hbm, u_in), (flow_hbm, flow_in), (imb_hbm, imb_in)))
        for k in range(K)
    ]
    for copy in fetches:
        copy.start()

    def gather(ref, *index):
        rows = pl.ds(index[-1], SUBS, stride=T)
        return jnp.concatenate([ref[(k,) + index[:-1] + (rows, slice(None))] for k in range(K)], axis=1)

    def scatter(ref, value, *index):
        rows = pl.ds(index[-1], SUBS, stride=T)
        for k in range(K):
            ref[(k,) + index[:-1] + (rows, slice(None))] = value[:, k * LANES:(k + 1) * LANES]

    barrier = pltpu.get_barrier_semaphore()

    def coords(offset):
        other = lax.rem(me + offset, n)
        return (other // nx, lax.rem(other, nx))

    def greet(k, c):
        pl.semaphore_signal(barrier, inc=1, device_id=coords(k), device_id_type=MESH)
        return c

    lax.fori_loop(1, n, greet, 0)

    lane = lax.broadcasted_iota(jnp.int32, (SUBS, LANES), 1)
    sub = lax.broadcasted_iota(jnp.int32, (SUBS, LANES), 0)
    subw = lax.broadcasted_iota(jnp.int32, (SUBS, C), 0)
    group, within = lane // T, lax.rem(lane, T)
    lane1, within1 = lane[0:1], within[0:1]

    def wide(x):
        return jnp.concatenate([x] * (C // LANES), axis=1)

    def row8(x, width):
        return jnp.broadcast_to(x, (SUBS, width))

    def to_left(x, entering):
        r = pltpu.roll(x, C - 1, 1)
        lanes = lax.broadcasted_iota(jnp.int32, entering.shape, 1)
        tail = jnp.where(lanes == LANES - 1, entering, r[:, C - LANES:])
        return jnp.concatenate([r[:, : C - LANES], tail], axis=1)

    def to_right(x, entering):
        r = pltpu.roll(x, 1, 1)
        head = jnp.where(lane == 0, entering, r[:, :LANES])
        return jnp.concatenate([head, r[:, LANES:]], axis=1)

    def pack_first(acc, x, t):
        v = x[:, :LANES]
        return jnp.where(lane == t, pltpu.roll(v, t, 1) if t else v, acc)

    def pack_last(acc, x, t):
        v = pltpu.roll(x[:, C - LANES:], (t + 1) % LANES, 1)
        return jnp.where(lane == t, v, acc)

    def turned(x, by):
        return x if isinstance(by, int) and by == 0 else pltpu.roll(x, by, 1)

    def place(acc, packed, p):
        return jnp.where(group == p, turned(packed, p * T), acc)

    def remote(src, dst, ssem, rsem, where):
        return pltpu.make_async_remote_copy(
            src_ref=src, dst_ref=dst, send_sem=ssem, recv_sem=rsem, device_id=where, device_id_type=MESH
        )

    def halos(slot, g):
        rows = [
            (ok_to, ok_from, remote(row_send.at[slot, k, g], row_recv.at[slot, k, g], halo_ssem.at[slot, k, g], halo_rsem.at[slot, k, g], (gy + d, gx)))
            for k, d, ok_to, ok_from in ((0, -1, up, down), (1, 1, down, up))
        ]
        cols = [
            (ok_to, ok_from, remote(col_send.at[slot, k, g], col_recv.at[slot, k, g], halo_ssem.at[slot, 2 + k, g], halo_rsem.at[slot, 2 + k, g], (gy, gx + d)))
            for k, d, ok_to, ok_from in ((0, -1, left, right), (1, 1, right, left))
        ]
        return rows + cols

    def extras():
        return [
            (down, up, remote(ext_row, ext_row_in, ext_ssem.at[0], ext_rsem.at[0], (gy + 1, gx))),
            (right, left, remote(ext_col, ext_col_in, ext_ssem.at[1], ext_rsem.at[1], (gy, gx + 1))),
        ]

    def start_all(copies):
        for ok_to, _, copy in copies:
            @pl.when(ok_to)
            def _(copy=copy):
                copy.start()

    def wait_all(copies):
        for ok_to, ok_from, copy in copies:
            @pl.when(ok_from)
            def _(copy=copy):
                copy.wait_recv()

            @pl.when(ok_to)
            def _(copy=copy):
                copy.wait_send()

    def send_message(slot, g, row):
        msg_send[slot, g] = row
        msg_recv[slot, g, me] = row

        def send(j, c):
            y = jnp.where(gy < ny // 2, ny - 1 - j, j)
            for x in range(nx):
                @pl.when(jnp.logical_or(y != gy, gx != x))
                def _():
                    remote(
                        msg_send.at[slot, g], msg_recv.at[slot, g, me], msg_ssem.at[slot, g], msg_rsem.at[slot, g], (y, x)
                    ).start()
            return c

        lax.fori_loop(0, ny, send, 0)

    def wait_message(slot, g):
        whole = msg_recv.at[slot, g, pl.ds(0, n - 1)]
        pltpu.make_async_copy(whole, whole, msg_rsem.at[slot, g]).wait()
        pltpu.make_async_copy(whole, whole, msg_ssem.at[slot, g]).wait()

    def total_rows(slot, g):
        parts = [msg_recv[slot, g, k] for k in range(n)]
        while len(parts) > 1:
            parts = [sum(parts[k + 1:k + 2], parts[k]) for k in range(0, len(parts), 2)]
        total = row8(parts[0], LANES)
        pick = jnp.where(sub < gp, sub * T + 1, (sub - gp) * T + 2)
        return row8_lanes(jnp.sum(jnp.where(lane == pick, total, 0.0), axis=1, keepdims=True))

    def each(body, init):
        return lax.fori_loop(0, gp, body, init) if gp > 1 else body(0, init)

    def row8_lanes(x):
        return jnp.broadcast_to(x, (SUBS, LANES))

    def message(first, last, sums_a, sums_b):
        return jnp.where(
            within1 == T - 1, first[SUBS - 1:SUBS],
            jnp.where(within1 == 0, last[0:1], jnp.where(within1 == 1, sums_a, sums_b)),
        )

    ones = jnp.ones((SUBS, LANES), f32)
    for copy in fetches:
        copy.wait()
    for t in range(T):
        CO[t] = gather(cost_in, t)

    def load(g, c):
        def problem(p, carry):
            packs = [ones] * 5
            q = g * gp + p
            for t in range(T):
                a, b = gather(flow_in, 0, q, t), gather(flow_in, 1, q, t)
                u = gather(u_in, q, t)
                A[q, t] = a
                B[q, t] = b
                U[q, t] = u
                IM[q, t] = gather(imb_in, q, t)
                packs[0] = pack_first(packs[0], u, t)
                for k, x in ((1, u), (2, a), (3, b), (4, CO[t])):
                    packs[k] = pack_last(packs[k], x, t)
                if t == 0:
                    row_send[0, 0, g, pl.ds(p, 1), :] = u[0:1]
                if t == T - 1:
                    row_send[0, 1, g, pl.ds(p, 1), :] = u[SUBS - 1:]
                    ext_row[0, g, pl.ds(p, 1), :] = a[SUBS - 1:]
                    ext_row[1, g, pl.ds(p, 1), :] = b[SUBS - 1:]
                    ext_row[2, g, pl.ds(p, 1), :] = CO[t][SUBS - 1:]
            return tuple(place(c, x, p) for c, x in zip(carry, packs))

        first, last, last_a, last_b, last_c = each(problem, (ones,) * 5)
        col_send[0, 0, g] = first
        col_send[0, 1, g] = last
        ext_col[0, g] = last_a
        ext_col[1, g] = last_b
        ext_col[2, g] = last_c
        return c

    lax.fori_loop(0, G, load, 0)
    tau_ref[...] = jnp.full(tau_ref.shape, initial_step, f32)
    sig_ref[...] = jnp.full(sig_ref.shape, initial_step, f32)

    for missing, refs in (
        (jnp.logical_not(down), [row_recv.at[s, 0] for s in range(2)]),
        (jnp.logical_not(up), [row_recv.at[s, 1] for s in range(2)] + [ext_row_in]),
        (jnp.logical_not(right), [col_recv.at[s, 0] for s in range(2)]),
        (jnp.logical_not(left), [col_recv.at[s, 1] for s in range(2)] + [ext_col_in]),
    ):
        @pl.when(missing)
        def _(refs=refs):
            for ref in refs:
                ref[...] = jnp.zeros(ref.shape, f32)

    pl.semaphore_wait(barrier, n - 1)
    start_all(extras())

    def announce(g, c):
        start_all(halos(0, g))
        send_message(0, g, message(col_send[0, 0, g], col_send[0, 1, g], ones[0:1], ones[0:1]))
        return c

    lax.fori_loop(0, G, announce, 0)
    wait_all(extras())
    for k in range(2):
        for g in range(G):
            grow[g, k] = ext_row_in[k, g]
            gcol[g, k] = ext_col_in[k, g]

    def above_first(a_last, g, p):
        ghost = row8(grow[g, 0, pl.ds(p, 1), :], C)
        return jnp.where(subw == 0, ghost, pltpu.roll(a_last, 1, 0))

    def shortfall(p, t, a, a_above, b, gb):
        b_left = to_right(b, pltpu.roll(gb, (LANES - t) % LANES, 1))
        return ((a - a_above) + (b - b_left)) - IM[p, t]

    def ghost_flux(g, p):
        return turned(gcol[g, 1], (LANES - p * T) % LANES)

    def begin(g, c):
        def problem(p, c):
            q = g * gp + p
            gb = ghost_flux(g, p)
            for t in range(T):
                above = A[q, t - 1] if t else above_first(A[q, T - 1], g, p)
                R[q, t] = shortfall(q, t, A[q, t], above, B[q, t], gb)
            return c

        return each(problem, c)

    lax.fori_loop(0, G, begin, 0)

    results = [
        pltpu.make_async_copy(src.at[k], column(dst, k), out_sem.at[i, k])
        for i, (src, dst) in enumerate(((flow_in, flow_hbm_out), (u_in, u_hbm_out)))
        for k in range(K)
    ]

    def shrink(va, vb, t):
        f = jnp.maximum(1.0 - t * lax.rsqrt(va * va + vb * vb), 0.0)
        return f * va, f * vb

    def ghosts(slot, g):
        u = row_recv[slot, 1, g]
        sub_p, lane_p = sub[:gp], lane[:gp]
        ok = jnp.logical_and(up, right)
        corner = msg_recv[slot, g, jnp.where(ok, me - nx + 1, me)]
        corner = jnp.where(ok, corner, jnp.zeros_like(corner))
        corner = jnp.broadcast_to(corner, (gp, LANES))
        corner = jnp.sum(jnp.where(lane_p == sub_p * T + T - 1, corner, 0.0), axis=1, keepdims=True)
        u_right = to_left(u, jnp.broadcast_to(corner, (gp, LANES)))
        rate = wide(tau_ref[g, 0:gp])
        a2, b2 = shrink(
            grow[g, 0] + rate * (row_send[slot, 0, g] - u), grow[g, 1] + rate * (u_right - u), rate * ext_row_in[2, g]
        )
        grow[g, 0] = jnp.where(up, a2, jnp.zeros_like(a2))
        grow[g, 1] = jnp.where(up, b2, jnp.zeros_like(b2))
        u = col_recv[slot, 1, g]
        ok = jnp.logical_and(down, left)
        corner = msg_recv[slot, g, jnp.where(ok, me + nx - 1, me)]
        corner = jnp.where(ok, corner, jnp.zeros_like(corner))
        turn = jnp.where(sub == SUBS - 1, row8(corner, LANES), pltpu.roll(u, SUBS - 1, 0))
        u_down = jnp.where(within == T - 1, pltpu.roll(turn, T - 1, 1), pltpu.roll(u, LANES - 1, 1))
        rate = row8(tau_ref[g, 0:1], LANES)
        for p in range(1, gp):
            rate = jnp.where(group == p, row8(tau_ref[g, p:p + 1], LANES), rate)
        a2, b2 = shrink(
            gcol[g, 0] + rate * (u_down - u), gcol[g, 1] + rate * (col_send[slot, 0, g] - u), rate * ext_col_in[2, g]
        )
        gcol[g, 0] = jnp.where(left, a2, jnp.zeros_like(a2))
        gcol[g, 1] = jnp.where(left, b2, jnp.zeros_like(b2))

    def sweep(i, g, slot, closing):
        other = 1 - slot
        wait_all(halos(slot, g))
        wait_message(slot, g)
        sums = total_rows(slot, g)
        primal, dual_sums = sums, pltpu.roll(sums, SUBS - gp, 0)
        s = jnp.sqrt(jnp.sqrt((primal + epsilon) / (dual_sums + epsilon)))
        s = jnp.where(i == 0, 1.0, s)
        tau_ref[g] = tau_ref[g] / s
        sig_ref[g] = sig_ref[g] * s
        ghosts(slot, g)

        def problem(p, carry):
            sums_a, sums_b, first, last = carry
            q = g * gp + p
            tau = wide(row8(tau_ref[g, pl.ds(p, 1), :], LANES))
            sigma = wide(row8(sig_ref[g, pl.ds(p, 1), :], LANES))
            gb = ghost_flux(g, p)
            hc = pltpu.roll(col_recv[slot, 0, g], LANES - 1 - p * T, 1)
            acc_p = jnp.zeros((SUBS, C), f32)
            acc_d = jnp.zeros((SUBS, C), f32)
            pack_f, pack_l = ones, ones

            def dual(t, a2, above, b2, u):
                nonlocal acc_p, acc_d, pack_f, pack_l
                r2 = shortfall(q, t, a2, above, b2, gb)
                change = sigma * (r2 + (r2 - R[q, t]))
                u2 = u + change
                if closing:
                    acc_d = acc_d + r2 * r2
                    scatter(u_in, u2, q, t)
                    return
                acc_d = acc_d + change * change
                R[q, t] = r2
                U[q, t] = u2
                pack_f = pack_first(pack_f, u2, t)
                pack_l = pack_last(pack_l, u2, t)
                if t == 0:
                    row_send[other, 0, g, pl.ds(p, 1), :] = u2[0:1]
                if t == T - 1:
                    row_send[other, 1, g, pl.ds(p, 1), :] = u2[SUBS - 1:]

            u_first = u = U[q, 0]
            for t in range(T):
                if t < T - 1:
                    u_down = U[q, t + 1]
                else:
                    below = row8(row_recv[slot, 0, g, pl.ds(p, 1), :], C)
                    u_down = jnp.where(subw == SUBS - 1, below, pltpu.roll(u_first, SUBS - 1, 0))
                u_right = to_left(u, pltpu.roll(hc, (LANES - t) % LANES, 1))
                a, b = A[q, t], B[q, t]
                a2, b2 = shrink(a + tau * (u_down - u), b + tau * (u_right - u), tau * CO[t])
                if closing:
                    scatter(flow_in, a2, 0, q, t)
                    scatter(flow_in, b2, 1, q, t)
                else:
                    A[q, t] = a2
                    B[q, t] = b2
                    da, db = a2 - a, b2 - b
                    acc_p = acc_p + (da * da + db * db)
                if t:
                    dual(t, a2, above, b2, u)
                else:
                    a_first, b_first = a2, b2
                above, u = a2, u_down
            dual(0, a_first, above_first(above, g, p), b_first, u_first)

            def settle(sums, acc):
                part = jnp.sum(jnp.sum(acc, axis=0, keepdims=True), axis=1, keepdims=True)
                return jnp.where(group[0:1] == p, jnp.broadcast_to(part, (1, LANES)), sums)

            sums_b = settle(sums_b, acc_d)
            if closing:
                return sums_a, sums_b, first, last
            return settle(sums_a, acc_p), sums_b, place(first, pack_f, p), place(last, pack_l, p)

        start = (ones[0:1], ones[0:1], ones, ones)
        sums_a, sums_b, first, last = each(problem, start)
        if not closing:
            col_send[other, 0, g] = first
            col_send[other, 1, g] = last
        send_message(other, g, message(first, last, sums_a, sums_b))
        if not closing:
            start_all(halos(other, g))

    def turn(i, c):
        def one(g, c):
            sweep(i, g, lax.rem(i, 2), False)
            return c

        return lax.fori_loop(0, G, one, c)

    lax.fori_loop(0, ITERS - 1, turn, 0)
    slot = (ITERS - 1) % 2

    def close(g, c):
        sweep(ITERS - 1, g, slot, True)
        return c

    lax.fori_loop(0, G, close, 0)
    for copy in results:
        copy.start()
    cells = T * SUBS * C * n
    for g in range(G):
        wait_message(1 - slot, g)
        res_out[g] = total_rows(1 - slot, g) / cells
    for copy in results:
        copy.wait()


def local(ny, nx, imbalance, flow, potential, cost):
    pairs, rows, cols = imbalance.shape
    T = rows // SUBS
    n = ny * nx
    assert 2 * pairs <= SUBS and pairs * T <= LANES and T >= 4
    G = GROUPS if pairs % GROUPS == 0 else 1
    gp = pairs // G
    f32 = jnp.float32
    block = (pairs, T, SUBS, cols)
    packed = (SUBS, LANES)
    K = cols // LANES
    hbm = pl.BlockSpec(memory_space=pltpu.HBM)
    flow_out, u_out, res = pl.pallas_call(
        functools.partial(kernel, ny, nx),
        out_shape=(
            jax.ShapeDtypeStruct(flow.shape, f32),
            jax.ShapeDtypeStruct(potential.shape, f32),
            jax.ShapeDtypeStruct((G,) + packed, f32),
        ),
        in_specs=[hbm] * 4,
        out_specs=(hbm, hbm, pl.BlockSpec(memory_space=pltpu.VMEM)),
        scratch_shapes=[
            pltpu.VMEM((K, pairs, rows, LANES), f32), pltpu.VMEM((K, 2, pairs, rows, LANES), f32),
            pltpu.VMEM((K, pairs, rows, LANES), f32), pltpu.VMEM((K, rows, LANES), f32),
            pltpu.VMEM(block, f32), pltpu.VMEM(block, f32), pltpu.VMEM(block, f32), pltpu.VMEM(block, f32),
            pltpu.VMEM(block, f32), pltpu.VMEM(block[1:], f32),
            pltpu.VMEM((G,) + packed, f32), pltpu.VMEM((G,) + packed, f32),
            pltpu.VMEM((2, 2, G, gp, cols), f32), pltpu.VMEM((2, 2, G) + packed, f32),
            pltpu.VMEM((2, 2, G, gp, cols), f32), pltpu.VMEM((2, 2, G) + packed, f32),
            pltpu.VMEM((2, G, 1, LANES), f32), pltpu.VMEM((2, G, n, 1, LANES), f32),
            pltpu.VMEM((3, G, gp, cols), f32), pltpu.VMEM((3, G) + packed, f32),
            pltpu.VMEM((3, G, gp, cols), f32), pltpu.VMEM((3, G) + packed, f32),
            pltpu.VMEM((G, 2, gp, cols), f32), pltpu.VMEM((G, 2) + packed, f32),
            pltpu.SemaphoreType.DMA((2, 4, G)), pltpu.SemaphoreType.DMA((2, 4, G)),
            pltpu.SemaphoreType.DMA((2, G)), pltpu.SemaphoreType.DMA((2, G)),
            pltpu.SemaphoreType.DMA((2,)), pltpu.SemaphoreType.DMA((2,)),
            pltpu.SemaphoreType.DMA((4, K)), pltpu.SemaphoreType.DMA((2, K)),
        ],
        compiler_params=pltpu.CompilerParams(
            collective_id=0, has_side_effects=True, vmem_limit_bytes=48 * 1024 * 1024
        ),
    )(imbalance, flow, potential, cost)
    return flow_out, u_out, res[:, gp:2 * gp, 0].reshape(pairs)


def solution(mesh):
    placed = (P(None, "gy", "gx"), P(None, None, "gy", "gx"), P(None, "gy", "gx"), P("gy", "gx"))
    return jax.shard_map(
        functools.partial(local, mesh.shape["gy"], mesh.shape["gx"]),
        mesh=mesh,
        in_specs=placed,
        out_specs=(P(None, None, "gy", "gx"), P(None, "gy", "gx"), P()),
        check_vma=False,
    )
```

```python
import functools

import jax
import jax.numpy as jnp
from jax import lax
from jax.experimental import pallas as pl
from jax.experimental.pallas import tpu as pltpu
from jax.sharding import PartitionSpec as P

ITERS = 12
LANES = 128
GROUPS = 4
SUBS = 8

initial_step = 0.35
epsilon = 1e-06
MESH = pl.DeviceIdType.MESH


def kernel(
    ny, nx,
    imb_hbm, flow_hbm, u_hbm, cost_hbm,
    flow_hbm_out, u_hbm_out, res_out,
    imb_in, flow_in, u_in, cost_in,
    A, B, U, R, IM, CO,
    tau_ref, sig_ref,
    row_send, col_send, row_recv, col_recv, msg_send, msg_recv,
    ext_row, ext_col, ext_row_in, ext_col_in, grow, gcol,
    halo_ssem, halo_rsem, msg_ssem, msg_rsem, ext_ssem, ext_rsem, in_sem, out_sem,
):
    pairs, T, _, C = A.shape
    n = ny * nx
    G = grow.shape[0]
    gp = pairs // G
    gy, gx = lax.axis_index("gy"), lax.axis_index("gx")
    me = gy * nx + gx
    up, down, left, right = gy > 0, gy < ny - 1, gx > 0, gx < nx - 1
    f32 = jnp.float32

    K = C // LANES

    def column(ref, k):
        return ref.at[(slice(None),) * (len(ref.shape) - 1) + (pl.ds(k * LANES, LANES),)]

    fetches = [
        pltpu.make_async_copy(column(src, k), dst.at[k], in_sem.at[i, k])
        for i, (src, dst) in enumerate(((cost_hbm, cost_in), (u_hbm, u_in), (flow_hbm, flow_in), (imb_hbm, imb_in)))
        for k in range(K)
    ]
    for copy in fetches:
        copy.start()

    def gather(ref, *index):
        rows = pl.ds(index[-1], SUBS, stride=T)
        return jnp.concatenate([ref[(k,) + index[:-1] + (rows, slice(None))] for k in range(K)], axis=1)

    def scatter(ref, value, *index):
        rows = pl.ds(index[-1], SUBS, stride=T)
        for k in range(K):
            ref[(k,) + index[:-1] + (rows, slice(None))] = value[:, k * LANES:(k + 1) * LANES]

    barrier = pltpu.get_barrier_semaphore()

    def coords(offset):
        other = lax.rem(me + offset, n)
        return (other // nx, lax.rem(other, nx))

    def greet(k, c):
        pl.semaphore_signal(barrier, inc=1, device_id=coords(k), device_id_type=MESH)
        return c

    lax.fori_loop(1, n, greet, 0)

    lane = lax.broadcasted_iota(jnp.int32, (SUBS, LANES), 1)
    sub = lax.broadcasted_iota(jnp.int32, (SUBS, LANES), 0)
    subw = lax.broadcasted_iota(jnp.int32, (SUBS, C), 0)
    group, within = lane // T, lax.rem(lane, T)
    lane1, within1 = lane[0:1], within[0:1]

    def wide(x):
        return jnp.concatenate([x] * (C // LANES), axis=1)

    def row8(x, width):
        return jnp.broadcast_to(x, (SUBS, width))

    def to_left(x, entering):
        r = pltpu.roll(x, C - 1, 1)
        lanes = lax.broadcasted_iota(jnp.int32, entering.shape, 1)
        tail = jnp.where(lanes == LANES - 1, entering, r[:, C - LANES:])
        return jnp.concatenate([r[:, : C - LANES], tail], axis=1)

    def to_right(x, entering):
        r = pltpu.roll(x, 1, 1)
        head = jnp.where(lane == 0, entering, r[:, :LANES])
        return jnp.concatenate([head, r[:, LANES:]], axis=1)

    def pack_first(acc, x, t):
        v = x[:, :LANES]
        return jnp.where(lane == t, pltpu.roll(v, t, 1) if t else v, acc)

    def pack_last(acc, x, t):
        v = pltpu.roll(x[:, C - LANES:], (t + 1) % LANES, 1)
        return jnp.where(lane == t, v, acc)

    def turned(x, by):
        return x if isinstance(by, int) and by == 0 else pltpu.roll(x, by, 1)

    def place(acc, packed, p):
        return jnp.where(group == p, turned(packed, p * T), acc)

    def remote(src, dst, ssem, rsem, where):
        return pltpu.make_async_remote_copy(
            src_ref=src, dst_ref=dst, send_sem=ssem, recv_sem=rsem, device_id=where, device_id_type=MESH
        )

    def halos(slot, g):
        rows = [
            (ok_to, ok_from, remote(row_send.at[slot, k, g], row_recv.at[slot, k, g], halo_ssem.at[slot, k, g], halo_rsem.at[slot, k, g], (gy + d, gx)))
            for k, d, ok_to, ok_from in ((0, -1, up, down), (1, 1, down, up))
        ]
        cols = [
            (ok_to, ok_from, remote(col_send.at[slot, k, g], col_recv.at[slot, k, g], halo_ssem.at[slot, 2 + k, g], halo_rsem.at[slot, 2 + k, g], (gy, gx + d)))
            for k, d, ok_to, ok_from in ((0, -1, left, right), (1, 1, right, left))
        ]
        return rows + cols

    def extras():
        return [
            (down, up, remote(ext_row, ext_row_in, ext_ssem.at[0], ext_rsem.at[0], (gy + 1, gx))),
            (right, left, remote(ext_col, ext_col_in, ext_ssem.at[1], ext_rsem.at[1], (gy, gx + 1))),
        ]

    def start_all(copies):
        for ok_to, _, copy in copies:
            @pl.when(ok_to)
            def _(copy=copy):
                copy.start()

    def wait_all(copies):
        for ok_to, ok_from, copy in copies:
            @pl.when(ok_from)
            def _(copy=copy):
                copy.wait_recv()

            @pl.when(ok_to)
            def _(copy=copy):
                copy.wait_send()

    def send_message(slot, g, row):
        msg_send[slot, g] = row
        msg_recv[slot, g, me] = row

        for j in range(ny):
            y = jnp.where(gy < ny // 2, ny - 1 - j, j)
            for x in range(nx):
                @pl.when(jnp.logical_or(y != gy, gx != x))
                def _():
                    remote(
                        msg_send.at[slot, g], msg_recv.at[slot, g, me], msg_ssem.at[slot, g], msg_rsem.at[slot, g], (y, x)
                    ).start()

    def wait_message(slot, g):
        whole = msg_recv.at[slot, g, pl.ds(0, n - 1)]
        pltpu.make_async_copy(whole, whole, msg_rsem.at[slot, g]).wait()
        pltpu.make_async_copy(whole, whole, msg_ssem.at[slot, g]).wait()

    def total_rows(slot, g):
        parts = [msg_recv[slot, g, k] for k in range(n)]
        while len(parts) > 1:
            parts = [sum(parts[k + 1:k + 2], parts[k]) for k in range(0, len(parts), 2)]
        total = row8(parts[0], LANES)
        pick = jnp.where(sub < gp, sub * T + 1, (sub - gp) * T + 2)
        return row8_lanes(jnp.sum(jnp.where(lane == pick, total, 0.0), axis=1, keepdims=True))

    def each(body, init):
        return lax.fori_loop(0, gp, body, init) if gp > 1 else body(0, init)

    def row8_lanes(x):
        return jnp.broadcast_to(x, (SUBS, LANES))

    def message(first, last, sums_a, sums_b):
        return jnp.where(
            within1 == T - 1, first[SUBS - 1:SUBS],
            jnp.where(within1 == 0, last[0:1], jnp.where(within1 == 1, sums_a, sums_b)),
        )

    ones = jnp.ones((SUBS, LANES), f32)
    for copy in fetches:
        copy.wait()
    for t in range(T):
        CO[t] = gather(cost_in, t)

    def load(g, c):
        def problem(p, carry):
            packs = [ones] * 5
            q = g * gp + p
            for t in range(T):
                a, b = gather(flow_in, 0, q, t), gather(flow_in, 1, q, t)
                u = gather(u_in, q, t)
                A[q, t] = a
                B[q, t] = b
                U[q, t] = u
                IM[q, t] = gather(imb_in, q, t)
                packs[0] = pack_first(packs[0], u, t)
                for k, x in ((1, u), (2, a), (3, b), (4, CO[t])):
                    packs[k] = pack_last(packs[k], x, t)
                if t == 0:
                    row_send[0, 0, g, pl.ds(p, 1), :] = u[0:1]
                if t == T - 1:
                    row_send[0, 1, g, pl.ds(p, 1), :] = u[SUBS - 1:]
                    ext_row[0, g, pl.ds(p, 1), :] = a[SUBS - 1:]
                    ext_row[1, g, pl.ds(p, 1), :] = b[SUBS - 1:]
                    ext_row[2, g, pl.ds(p, 1), :] = CO[t][SUBS - 1:]
            return tuple(place(c, x, p) for c, x in zip(carry, packs))

        first, last, last_a, last_b, last_c = each(problem, (ones,) * 5)
        col_send[0, 0, g] = first
        col_send[0, 1, g] = last
        ext_col[0, g] = last_a
        ext_col[1, g] = last_b
        ext_col[2, g] = last_c
        return c

    lax.fori_loop(0, G, load, 0)
    tau_ref[...] = jnp.full(tau_ref.shape, initial_step, f32)
    sig_ref[...] = jnp.full(sig_ref.shape, initial_step, f32)

    for missing, refs in (
        (jnp.logical_not(down), [row_recv.at[s, 0] for s in range(2)]),
        (jnp.logical_not(up), [row_recv.at[s, 1] for s in range(2)] + [ext_row_in]),
        (jnp.logical_not(right), [col_recv.at[s, 0] for s in range(2)]),
        (jnp.logical_not(left), [col_recv.at[s, 1] for s in range(2)] + [ext_col_in]),
    ):
        @pl.when(missing)
        def _(refs=refs):
            for ref in refs:
                ref[...] = jnp.zeros(ref.shape, f32)

    pl.semaphore_wait(barrier, n - 1)
    start_all(extras())

    def corners(g):
        return [
            (ok_to, ok_from, remote(msg_send.at[0, g], msg_recv.at[0, g, me], msg_ssem.at[2 + k, g], msg_rsem.at[2 + k, g], (gy + dy, gx + dx)))
            for k, dy, dx, ok_to, ok_from in (
                (0, -1, 1, jnp.logical_and(up, right), jnp.logical_and(down, left)),
                (1, 1, -1, jnp.logical_and(down, left), jnp.logical_and(up, right)),
            )
        ]

    def announce(g, c):
        row = message(col_send[0, 0, g], col_send[0, 1, g], ones[0:1], ones[0:1])
        msg_send[0, g] = row
        start_all(halos(0, g) + corners(g))
        return c

    lax.fori_loop(0, G, announce, 0)
    wait_all(extras())
    for k in range(2):
        for g in range(G):
            grow[g, k] = ext_row_in[k, g]
            gcol[g, k] = ext_col_in[k, g]

    def above_first(a_last, g, p):
        ghost = row8(grow[g, 0, pl.ds(p, 1), :], C)
        return jnp.where(subw == 0, ghost, pltpu.roll(a_last, 1, 0))

    def shortfall(p, t, a, a_above, b, gb):
        b_left = to_right(b, pltpu.roll(gb, (LANES - t) % LANES, 1))
        return ((a - a_above) + (b - b_left)) - IM[p, t]

    def ghost_flux(g, p):
        return turned(gcol[g, 1], (LANES - p * T) % LANES)

    def begin(g, c):
        def problem(p, c):
            q = g * gp + p
            gb = ghost_flux(g, p)
            for t in range(T):
                above = A[q, t - 1] if t else above_first(A[q, T - 1], g, p)
                R[q, t] = shortfall(q, t, A[q, t], above, B[q, t], gb)
            return c

        return each(problem, c)

    lax.fori_loop(0, G, begin, 0)

    def settled(g, c):
        wait_all(halos(0, g) + corners(g))
        return c

    lax.fori_loop(0, G, settled, 0)

    results = [
        pltpu.make_async_copy(src.at[k], column(dst, k), out_sem.at[i, k])
        for i, (src, dst) in enumerate(((flow_in, flow_hbm_out), (u_in, u_hbm_out)))
        for k in range(K)
    ]

    def shrink(va, vb, t):
        f = jnp.maximum(1.0 - t * lax.rsqrt(va * va + vb * vb), 0.0)
        return f * va, f * vb

    def ghosts(slot, g):
        u = row_recv[slot, 1, g]
        sub_p, lane_p = sub[:gp], lane[:gp]
        ok = jnp.logical_and(up, right)
        corner = msg_recv[slot, g, jnp.where(ok, me - nx + 1, me)]
        corner = jnp.where(ok, corner, jnp.zeros_like(corner))
        corner = jnp.broadcast_to(corner, (gp, LANES))
        corner = jnp.sum(jnp.where(lane_p == sub_p * T + T - 1, corner, 0.0), axis=1, keepdims=True)
        u_right = to_left(u, jnp.broadcast_to(corner, (gp, LANES)))
        rate = wide(tau_ref[g, 0:gp])
        a2, b2 = shrink(
            grow[g, 0] + rate * (row_send[slot, 0, g] - u), grow[g, 1] + rate * (u_right - u), rate * ext_row_in[2, g]
        )
        grow[g, 0] = jnp.where(up, a2, jnp.zeros_like(a2))
        grow[g, 1] = jnp.where(up, b2, jnp.zeros_like(b2))
        u = col_recv[slot, 1, g]
        ok = jnp.logical_and(down, left)
        corner = msg_recv[slot, g, jnp.where(ok, me + nx - 1, me)]
        corner = jnp.where(ok, corner, jnp.zeros_like(corner))
        turn = jnp.where(sub == SUBS - 1, row8(corner, LANES), pltpu.roll(u, SUBS - 1, 0))
        u_down = jnp.where(within == T - 1, pltpu.roll(turn, T - 1, 1), pltpu.roll(u, LANES - 1, 1))
        rate = row8(tau_ref[g, 0:1], LANES)
        for p in range(1, gp):
            rate = jnp.where(group == p, row8(tau_ref[g, p:p + 1], LANES), rate)
        a2, b2 = shrink(
            gcol[g, 0] + rate * (u_down - u), gcol[g, 1] + rate * (col_send[slot, 0, g] - u), rate * ext_col_in[2, g]
        )
        gcol[g, 0] = jnp.where(left, a2, jnp.zeros_like(a2))
        gcol[g, 1] = jnp.where(left, b2, jnp.zeros_like(b2))

    def adapt(slot, g):
        wait_all(halos(slot, g))
        wait_message(slot, g)
        sums = total_rows(slot, g)
        primal, dual_sums = sums, pltpu.roll(sums, SUBS - gp, 0)
        s = jnp.sqrt(jnp.sqrt((primal + epsilon) / (dual_sums + epsilon)))
        tau_ref[g] = tau_ref[g] / s
        sig_ref[g] = sig_ref[g] * s

    def sweep(g, slot, closing):
        other = 1 - slot
        ghosts(slot, g)

        def problem(p, carry):
            sums_a, sums_b, first, last = carry
            q = g * gp + p
            tau = wide(row8(tau_ref[g, pl.ds(p, 1), :], LANES))
            sigma = wide(row8(sig_ref[g, pl.ds(p, 1), :], LANES))
            gb = ghost_flux(g, p)
            hc = pltpu.roll(col_recv[slot, 0, g], LANES - 1 - p * T, 1)
            acc_p = jnp.zeros((SUBS, C), f32)
            acc_d = jnp.zeros((SUBS, C), f32)
            pack_f, pack_l = ones, ones

            def dual(t, a2, above, b2, u):
                nonlocal acc_p, acc_d, pack_f, pack_l
                r2 = shortfall(q, t, a2, above, b2, gb)
                change = sigma * (r2 + (r2 - R[q, t]))
                u2 = u + change
                if closing:
                    acc_d = acc_d + r2 * r2
                    scatter(u_in, u2, q, t)
                    return
                acc_d = acc_d + change * change
                R[q, t] = r2
                U[q, t] = u2
                pack_f = pack_first(pack_f, u2, t)
                pack_l = pack_last(pack_l, u2, t)
                if t == 0:
                    row_send[other, 0, g, pl.ds(p, 1), :] = u2[0:1]
                if t == T - 1:
                    row_send[other, 1, g, pl.ds(p, 1), :] = u2[SUBS - 1:]

            u_first = u = U[q, 0]
            for t in range(T):
                if t < T - 1:
                    u_down = U[q, t + 1]
                else:
                    below = row8(row_recv[slot, 0, g, pl.ds(p, 1), :], C)
                    u_down = jnp.where(subw == SUBS - 1, below, pltpu.roll(u_first, SUBS - 1, 0))
                u_right = to_left(u, pltpu.roll(hc, (LANES - t) % LANES, 1))
                a, b = A[q, t], B[q, t]
                a2, b2 = shrink(a + tau * (u_down - u), b + tau * (u_right - u), tau * CO[t])
                if closing:
                    scatter(flow_in, a2, 0, q, t)
                    scatter(flow_in, b2, 1, q, t)
                else:
                    A[q, t] = a2
                    B[q, t] = b2
                    da, db = a2 - a, b2 - b
                    acc_p = acc_p + (da * da + db * db)
                if t:
                    dual(t, a2, above, b2, u)
                else:
                    a_first, b_first = a2, b2
                above, u = a2, u_down
            dual(0, a_first, above_first(above, g, p), b_first, u_first)

            def settle(sums, acc):
                part = jnp.sum(jnp.sum(acc, axis=0, keepdims=True), axis=1, keepdims=True)
                return jnp.where(group[0:1] == p, jnp.broadcast_to(part, (1, LANES)), sums)

            sums_b = settle(sums_b, acc_d)
            if closing:
                return sums_a, sums_b, first, last
            return settle(sums_a, acc_p), sums_b, place(first, pack_f, p), place(last, pack_l, p)

        start = (ones[0:1], ones[0:1], ones, ones)
        sums_a, sums_b, first, last = each(problem, start)
        if not closing:
            col_send[other, 0, g] = first
            col_send[other, 1, g] = last
        send_message(other, g, message(first, last, sums_a, sums_b))
        if not closing:
            start_all(halos(other, g))

    def turn(i, c):
        slot = lax.rem(i, 2)

        def one(g, c):
            @pl.when(i > 0)
            def _():
                adapt(slot, g)

            sweep(g, slot, False)
            return c

        return lax.fori_loop(0, G, one, c)

    lax.fori_loop(0, ITERS - 1, turn, 0)
    slot = (ITERS - 1) % 2

    def close(g, c):
        adapt(slot, g)
        sweep(g, slot, True)
        return c

    lax.fori_loop(0, G, close, 0)
    for copy in results:
        copy.start()
    cells = T * SUBS * C * n
    for g in range(G):
        wait_message(1 - slot, g)
        res_out[g] = total_rows(1 - slot, g) / cells
    for copy in results:
        copy.wait()


def local(ny, nx, imbalance, flow, potential, cost):
    pairs, rows, cols = imbalance.shape
    T = rows // SUBS
    n = ny * nx
    assert 2 * pairs <= SUBS and pairs * T <= LANES and T >= 4
    G = GROUPS if pairs % GROUPS == 0 else 1
    gp = pairs // G
    f32 = jnp.float32
    block = (pairs, T, SUBS, cols)
    packed = (SUBS, LANES)
    K = cols // LANES
    hbm = pl.BlockSpec(memory_space=pltpu.HBM)
    flow_out, u_out, res = pl.pallas_call(
        functools.partial(kernel, ny, nx),
        out_shape=(
            jax.ShapeDtypeStruct(flow.shape, f32),
            jax.ShapeDtypeStruct(potential.shape, f32),
            jax.ShapeDtypeStruct((G,) + packed, f32),
        ),
        in_specs=[hbm] * 4,
        out_specs=(hbm, hbm, pl.BlockSpec(memory_space=pltpu.VMEM)),
        scratch_shapes=[
            pltpu.VMEM((K, pairs, rows, LANES), f32), pltpu.VMEM((K, 2, pairs, rows, LANES), f32),
            pltpu.VMEM((K, pairs, rows, LANES), f32), pltpu.VMEM((K, rows, LANES), f32),
            pltpu.VMEM(block, f32), pltpu.VMEM(block, f32), pltpu.VMEM(block, f32), pltpu.VMEM(block, f32),
            pltpu.VMEM(block, f32), pltpu.VMEM(block[1:], f32),
            pltpu.VMEM((G,) + packed, f32), pltpu.VMEM((G,) + packed, f32),
            pltpu.VMEM((2, 2, G, gp, cols), f32), pltpu.VMEM((2, 2, G) + packed, f32),
            pltpu.VMEM((2, 2, G, gp, cols), f32), pltpu.VMEM((2, 2, G) + packed, f32),
            pltpu.VMEM((2, G, 1, LANES), f32), pltpu.VMEM((2, G, n, 1, LANES), f32),
            pltpu.VMEM((3, G, gp, cols), f32), pltpu.VMEM((3, G) + packed, f32),
            pltpu.VMEM((3, G, gp, cols), f32), pltpu.VMEM((3, G) + packed, f32),
            pltpu.VMEM((G, 2, gp, cols), f32), pltpu.VMEM((G, 2) + packed, f32),
            pltpu.SemaphoreType.DMA((2, 4, G)), pltpu.SemaphoreType.DMA((2, 4, G)),
            pltpu.SemaphoreType.DMA((4, G)), pltpu.SemaphoreType.DMA((4, G)),
            pltpu.SemaphoreType.DMA((2,)), pltpu.SemaphoreType.DMA((2,)),
            pltpu.SemaphoreType.DMA((4, K)), pltpu.SemaphoreType.DMA((2, K)),
        ],
        compiler_params=pltpu.CompilerParams(
            collective_id=0, has_side_effects=True, vmem_limit_bytes=48 * 1024 * 1024
        ),
    )(*(pltpu.with_memory_space_constraint(x, pltpu.HBM) for x in (imbalance, flow, potential, cost)))
    return flow_out, u_out, res[:, gp:2 * gp, 0].reshape(pairs)


def solution(mesh):
    placed = (P(None, "gy", "gx"), P(None, None, "gy", "gx"), P(None, "gy", "gx"), P("gy", "gx"))
    return jax.shard_map(
        functools.partial(local, mesh.shape["gy"], mesh.shape["gx"]),
        mesh=mesh,
        in_specs=placed,
        out_specs=(P(None, None, "gy", "gx"), P(None, "gy", "gx"), P()),
        check_vma=False,
    )
```
